32 devices in a mesh: cfd: 16 (over z, x, core), ac: 2 (over y).
Axes of the slice: x: 2, y: 2, z: 4, core: 2. Of those that a mesh axis runs over, the one named last changes fastest.
Arguments:
- surface_raw: bfloat16 [5, 4096, 1024], P(None, ('cfd', 'ac')), may hold values from -6 to 6
- area_normals: bfloat16 [3, 4096], P(None, ('cfd', 'ac')), may hold values from -6 to 6
- kernel_weights: bfloat16 [2, 3, 2048, 4096], P(None, None, None, ('cfd', 'ac')), may hold values from -0.078125 to 0.078125
- block_map: int32 [2, 16, 16], P('ac', 'cfd'), may hold values from 0 to 15, as said below
- band_observers: int32 [16, 128], replicated, may hold values from 0 to 2047, as said below
- band_lags: int32 [16], replicated, may hold values from 0 to 511
Outputs:
- acoustic: float32 [2048, 512], P('cfd', 'ac')
The draws below stay inside these ranges and needn't reach their ends.
Inputs may be any that keep to these rules, and one draw needn't show every extreme that they name: block_map[j, s, :] is a permutation of 0 to 15 for every j and s. `band_observers`: every observer appears exactly once.
All inputs are finite; a program needn't handle non-finite values.
Results may differ from the reference program's by a relative error of at most 0.0042.
Values may be sent and summed in bfloat16 or wider, within the bound.
A program may use at most 64 MiB of HBM per device.

```python
import jax
import jax.numpy as jnp
from jax import lax

OBS = 2048
BANDS = 16
OBS_BAND = 128
TAPS = 2
BLOCK = 8
FACES = 4096
WINDOW = 1024
OUT_STEPS = 512
N_CFD = 16
N_AC = 2


def draw_band_observers(key, part):
    shuffled = jax.random.permutation(jax.random.fold_in(key, 11), OBS)
    return shuffled.astype(jnp.int32).reshape(BANDS, OBS // BANDS)


def draw_block_map(key, part):
    key_list = jax.random.split(jax.random.fold_in(key, 23), N_AC * N_CFD)
    orders = jax.vmap(lambda single_key: jax.random.permutation(single_key, N_CFD))(key_list)
    return orders.astype(jnp.int32).reshape(N_AC, N_CFD, N_CFD)


def set_ends(entries, stream_key, low, top_value):
    longest = entries.shape.index(max(entries.shape))
    spots = []
    for shift in (0, 1):
        where = [jax.random.randint(jax.random.fold_in(stream_key, axis), (), 0, length) for axis, length in enumerate(entries.shape)]
        where[longest] = (where[longest] + shift) % entries.shape[longest]
        spots.append(tuple(where))
    return entries.at[spots[0]].set(low).at[spots[1]].set(top_value)


def spiked(entries, rng, source, target, parts, factor):
    owner, partner = [(jnp.arange(entries.shape[axis_at]) // (entries.shape[axis_at] // parts)).reshape([-1 if axis == axis_at else 1 for axis in range(entries.ndim)]) for axis_at in (source, target)]
    chosen = jax.random.permutation(rng, parts)[partner]
    strong = (owner == chosen) | (owner == (partner + parts // 2) % parts)
    return jnp.where(strong, factor * entries, entries)


def block_scale(rng, shape, pieces, least, high):
    def one(dim, shards_of):
        draws = jax.random.uniform(jax.random.fold_in(jax.random.fold_in(rng, 6), dim), (shards_of,), jnp.float32, least / len(pieces), high / len(pieces))
        return jnp.repeat(jnp.exp(draws), shape[dim] // shards_of).reshape((-1,) + (1,) * (len(shape) - dim - 1))

    factor_of = one(*pieces[0])
    for cut in pieces[1:]:
        factor_of = factor_of * one(*cut)
    return factor_of


def gaussian(rng, dims, width, most, cuts=(), kind=jnp.bfloat16):
    values = width * jax.random.normal(rng, dims, jnp.float32)
    if cuts:
        values = values * block_scale(rng, dims, cuts, -0.22, 0.18)
    return jnp.clip(values, -most, most).astype(kind)


def gaussian_with(key, dims, scale, limit, cuts, heavy, held_as=jnp.bfloat16):
    result = scale * jax.random.normal(key, dims, jnp.float32)
    if cuts:
        result = result * block_scale(key, dims, cuts, -0.22, 0.18)
    return jnp.clip(spiked(result, jax.random.fold_in(key, 3), *heavy), -limit, limit).astype(held_as)


def setup_inputs(seed: int = 0) -> dict:
    seeds = jax.random.split(jax.random.key(seed), 7)
    surface_raw = gaussian(seeds[0], (5, FACES, WINDOW), 1.0, 6.0, ((1, 32),))
    area_normals = gaussian(seeds[1], (3, FACES), 1.0, 6.0, ((1, 32),))
    kernel_weights = gaussian_with(seeds[2], (TAPS, 3, OBS, FACES), (6 * FACES) ** -0.5, 0.078125, ((3, 32),), (3, 2, 32, 2.75))
    block_map = draw_block_map(jax.random.fold_in(seeds[6], 71), 0)
    band_observers = draw_band_observers(jax.random.fold_in(seeds[6], 71), 0)
    band_lags = set_ends(jax.random.randint(seeds[5], (BANDS,), 0, OUT_STEPS), jax.random.fold_in(seeds[5], 1), 0, OUT_STEPS - 1).astype(jnp.int32)
    return dict(surface_raw=surface_raw, area_normals=area_normals, kernel_weights=kernel_weights, block_map=block_map, band_observers=band_observers, band_lags=band_lags)


def thickness(surface, normals):
    along = surface[2].astype(jnp.float32) * normals[0].astype(jnp.float32)[:, None]
    along = along + surface[3].astype(jnp.float32) * normals[1].astype(jnp.float32)[:, None]
    along = along + surface[4].astype(jnp.float32) * normals[2].astype(jnp.float32)[:, None]
    return (surface[1].astype(jnp.float32) * along).astype(jnp.bfloat16)


def rates(series):
    step = series[:, 1:].astype(jnp.float32) - series[:, :-1].astype(jnp.float32)
    first = jnp.zeros((series.shape[0], 1), jnp.float32)
    return jnp.concatenate([first, step], axis=1).astype(jnp.bfloat16)


def reference(surface_raw, area_normals, kernel_weights, block_map, band_observers, band_lags):
    thick = thickness(surface_raw, area_normals)
    stacked = jnp.stack([thick, surface_raw[0]])
    shaped = stacked.reshape(2, N_CFD, N_AC, N_CFD, BLOCK, WINDOW)
    picks = jnp.transpose(block_map, (1, 0, 2))[None, :, :, :, None, None]
    moved = jnp.take_along_axis(shaped, picks, axis=3)
    moved = jnp.transpose(moved, (0, 3, 2, 1, 4, 5)).reshape(2, FACES, WINDOW)
    sources = jnp.stack([rates(moved[0]), rates(moved[1]), moved[1]])

    def one_band(acoustic, band_index):
        members = band_observers[band_index]
        delay = band_lags[band_index]
        start = (band_index * OBS_BAND).astype(jnp.int32)
        chosen = lax.dynamic_slice_in_dim(kernel_weights, start, OBS_BAND, 2).astype(jnp.float32)
        windows = jnp.stack([lax.dynamic_slice_in_dim(sources, (OUT_STEPS - delay - shift_step).astype(jnp.int32), OUT_STEPS, 2) for shift_step in range(TAPS)]).astype(jnp.float32)
        contribution = jnp.einsum("kcof,kcft->ot", chosen, windows, precision=lax.Precision.HIGHEST)
        return acoustic.at[members].set(contribution), None

    initial = jnp.zeros((OBS, OUT_STEPS), jnp.float32)
    acoustic, _ = lax.scan(one_band, initial, jnp.arange(BANDS, dtype=jnp.int32))
    return acoustic
```

```python
import functools

import jax
import jax.numpy as jnp
from jax import lax
from jax.experimental import pallas as pl
from jax.experimental.pallas import tpu as pltpu
from jax.sharding import PartitionSpec as P

LANES = 128


def prepare_kernel(src_ref, normals_ref, surface_ref, out_ref):
    along = surface_ref[2].astype(jnp.float32) * normals_ref[:, 0:1]
    along = along + surface_ref[3].astype(jnp.float32) * normals_ref[:, 1:2]
    along = along + surface_ref[4].astype(jnp.float32) * normals_ref[:, 2:3]
    thick = (surface_ref[1].astype(jnp.float32) * along).astype(jnp.bfloat16)
    both = jnp.concatenate([thick, surface_ref[0]], axis=0)
    rows = both.shape[0]
    column = lax.broadcasted_iota(jnp.int32, (rows, rows), 1)
    onehot = jnp.where(column == src_ref[...], 1.0, 0.0).astype(jnp.bfloat16)
    picked = jnp.dot(onehot, both, preferred_element_type=jnp.float32)
    out_ref[...] = picked.astype(jnp.bfloat16)


def prepare(surface_raw, area_normals, block_order):
    faces, steps = surface_raw.shape[1:]
    blocks = block_order.shape[0]
    size = faces // blocks
    src = (
        jnp.arange(2, dtype=jnp.int32)[None, :, None] * faces
        + block_order[:, None, None] * size
        + jnp.arange(size, dtype=jnp.int32)[None, None, :]
    ).reshape(2 * faces, 1)
    return pl.pallas_call(
        prepare_kernel,
        out_shape=jax.ShapeDtypeStruct((2 * faces, steps), jnp.bfloat16),
        name="prepare",
    )(src, area_normals.T.astype(jnp.float32), surface_raw)


def scatter_bands(lags_ref, ids_ref, arrived_ref, weights_ref, sources, band, rows):
    index = pl.program_id(0)
    taps, terms, width, faces = weights_ref.shape
    steps = sources.shape[1]
    out_len = steps // 2
    chunks = out_len // LANES

    @pl.when(index == 0)
    def _():
        series = arrived_ref[...].astype(jnp.float32)
        if len(arrived_ref.shape) == 4:
            thick = series[:, 0].reshape(faces, steps)
            pressure = series[:, 1].reshape(faces, steps)
        else:
            thick, pressure = series[:faces], series[faces:]
        step = lax.broadcasted_iota(jnp.int32, (faces, steps), 1)

        def rate(x):
            moved = jnp.where(step > 0, x - pltpu.roll(x, 1, 1), 0.0)
            return moved.astype(jnp.bfloat16).astype(jnp.float32)

        for c, x in enumerate((rate(thick), rate(pressure), pressure)):
            for k in range(taps):
                late = pltpu.roll(x, k, 1) if k else x
                sources[pl.ds((k * terms + c) * faces, faces), :] = late.astype(jnp.bfloat16)

    start = out_len - lags_ref[index]
    tile = jnp.minimum(start // LANES, steps // LANES - chunks - 1)
    rest = start - tile * LANES
    shift = lax.rem(LANES - rest, LANES)
    chosen = jnp.concatenate(
        [weights_ref[k, c] for k in range(taps) for c in range(terms)], axis=1
    )
    window = sources[:, pl.ds(pl.multiple_of(tile * LANES, LANES), out_len + LANES)]
    wide = jnp.dot(chosen, window, preferred_element_type=jnp.float32)
    lane = lax.broadcasted_iota(jnp.int32, (width, LANES), 1)
    parts = [
        pltpu.roll(wide[:, t * LANES : (t + 1) * LANES], shift, 1) for t in range(chunks + 1)
    ]
    for t in range(chunks):
        band[pl.ds(t, width, stride=chunks), :] = jnp.where(
            lane < LANES - rest, parts[t], parts[t + 1]
        )

    unroll = 16

    @pl.loop(0, width // unroll)
    def _(group):
        for m in range(unroll):
            slot = group * unroll + m
            place = ids_ref[index * width + slot]
            rows[pl.ds(pl.multiple_of(place * chunks, chunks), chunks), :] = band[
                pl.ds(pl.multiple_of(slot * chunks, chunks), chunks), :
            ]


def whole_kernel(lags_ref, ids_ref, arrived_ref, weights_ref, out_ref, sources, band, rows):
    scatter_bands(lags_ref, ids_ref, arrived_ref, weights_ref, sources, band, rows)
    observers, out_len = out_ref.shape
    chunks = out_len // LANES

    @pl.when(pl.program_id(0) == pl.num_programs(0) - 1)
    def _():
        for t in range(chunks):
            out_ref[:, t * LANES : (t + 1) * LANES] = rows[pl.ds(t, observers, stride=chunks), :]


def banded_call(kernel, outs, arrived, kernel_weights, band_observers, band_lags):
    taps, terms, observers, faces = kernel_weights.shape
    bands, width = band_observers.shape
    steps = arrived.shape[-1]
    chunks = steps // 2 // LANES
    rank = len(arrived.shape)
    return pl.pallas_call(
        kernel,
        out_shape=outs,
        grid_spec=pltpu.PrefetchScalarGridSpec(
            num_scalar_prefetch=2,
            grid=(bands,),
            in_specs=[
                pl.BlockSpec(arrived.shape, lambda b, *_: (0,) * rank),
                pl.BlockSpec((taps, terms, width, faces), lambda b, *_: (0, 0, b, 0)),
            ],
            out_specs=jax.tree.map(
                lambda o: pl.BlockSpec(o.shape, lambda b, *_: (0,) * len(o.shape)), outs
            ),
            scratch_shapes=[
                pltpu.VMEM((taps * terms * faces, steps), jnp.bfloat16),
                pltpu.VMEM((width * chunks, LANES), jnp.float32),
                pltpu.VMEM((observers * chunks, LANES), jnp.float32),
            ],
        ),
        compiler_params=pltpu.CompilerParams(dimension_semantics=("arbitrary",)),
        name="bands",
    )(band_lags, band_observers.reshape(-1), arrived, kernel_weights)


def local(surface_raw, area_normals, kernel_weights, block_map, band_observers, band_lags):
    blocks = lax.axis_size("cfd")
    faces, steps = surface_raw.shape[1:]
    size = faces // blocks
    outgoing = prepare(surface_raw, area_normals, block_map[0, 0])
    arrived = lax.all_to_all(outgoing, "cfd", split_axis=0, concat_axis=0, tiled=True)
    arrived = arrived.reshape(blocks, 2, size, steps)
    if size % 8:
        arrived = arrived.transpose(1, 0, 2, 3).reshape(2 * faces, steps)
    partial_value = banded_call(
        whole_kernel,
        jax.ShapeDtypeStruct((kernel_weights.shape[2], steps // 2), jnp.float32),
        arrived,
        kernel_weights,
        band_observers,
        band_lags,
    )
    reduced = lax.psum_scatter(partial_value, "cfd", scatter_dimension=0, tiled=True)
    return lax.psum_scatter(reduced, "ac", scatter_dimension=1, tiled=True)


def solution(mesh):
    placed = (
        P(None, ("cfd", "ac"), None),
        P(None, ("cfd", "ac")),
        P(None, None, None, ("cfd", "ac")),
        P("ac", "cfd", None),
        P(),
        P(),
    )
    return jax.shard_map(
        local, mesh=mesh, in_specs=placed, out_specs=P("cfd", "ac"), check_vma=False
    )
```

```python
import functools

import jax
import jax.numpy as jnp
from jax import lax
from jax.experimental import pallas as pl
from jax.experimental.pallas import tpu as pltpu
from jax.sharding import PartitionSpec as P

LANES = 128


def prepare_kernel(src_ref, normals_ref, surface_ref, out_ref):
    along = surface_ref[2].astype(jnp.float32) * normals_ref[:, 0:1]
    along = along + surface_ref[3].astype(jnp.float32) * normals_ref[:, 1:2]
    along = along + surface_ref[4].astype(jnp.float32) * normals_ref[:, 2:3]
    thick = (surface_ref[1].astype(jnp.float32) * along).astype(jnp.bfloat16)
    both = jnp.concatenate([thick, surface_ref[0]], axis=0)
    rows = both.shape[0]
    column = lax.broadcasted_iota(jnp.int32, (rows, rows), 1)
    onehot = jnp.where(column == src_ref[...], 1.0, 0.0).astype(jnp.bfloat16)
    picked = jnp.dot(onehot, both, preferred_element_type=jnp.float32)
    out_ref[...] = picked.astype(jnp.bfloat16)


def prepare(surface_raw, area_normals, block_order):
    faces, steps = surface_raw.shape[1:]
    blocks = block_order.shape[0]
    size = faces // blocks
    src = (
        jnp.arange(2, dtype=jnp.int32)[None, :, None] * faces
        + block_order[:, None, None] * size
        + jnp.arange(size, dtype=jnp.int32)[None, None, :]
    ).reshape(2 * faces, 1)
    return pl.pallas_call(
        prepare_kernel,
        out_shape=jax.ShapeDtypeStruct((2 * faces, steps), jnp.bfloat16),
        name="prepare",
    )(src, area_normals.T.astype(jnp.float32), surface_raw)


def scatter_bands(lags_ref, ids_ref, arrived_ref, weights_ref, sources, band, rows):
    index = pl.program_id(0)
    taps, terms, width, faces = weights_ref.shape
    steps = sources.shape[1]
    out_len = steps // 2
    chunks = out_len // LANES

    @pl.when(index == 0)
    def _():
        series = arrived_ref[...].astype(jnp.float32)
        if len(arrived_ref.shape) == 4:
            thick = series[:, 0].reshape(faces, steps)
            pressure = series[:, 1].reshape(faces, steps)
        else:
            thick, pressure = series[:faces], series[faces:]
        step = lax.broadcasted_iota(jnp.int32, (faces, steps), 1)

        def rate(x):
            moved = jnp.where(step > 0, x - pltpu.roll(x, 1, 1), 0.0)
            return moved.astype(jnp.bfloat16).astype(jnp.float32)

        for c, x in enumerate((rate(thick), rate(pressure), pressure)):
            for k in range(taps):
                late = pltpu.roll(x, k, 1) if k else x
                sources[pl.ds((k * terms + c) * faces, faces), :] = late.astype(jnp.bfloat16)

    start = out_len - lags_ref[index]
    tile = jnp.minimum(start // LANES, steps // LANES - chunks - 1)
    rest = start - tile * LANES
    shift = lax.rem(LANES - rest, LANES)
    chosen = jnp.concatenate(
        [weights_ref[k, c] for k in range(taps) for c in range(terms)], axis=1
    )
    window = sources[:, pl.ds(pl.multiple_of(tile * LANES, LANES), out_len + LANES)]
    wide = jnp.dot(chosen, window, preferred_element_type=jnp.float32)
    lane = lax.broadcasted_iota(jnp.int32, (width, LANES), 1)
    parts = [
        pltpu.roll(wide[:, t * LANES : (t + 1) * LANES], shift, 1) for t in range(chunks + 1)
    ]
    for t in range(chunks):
        band[pl.ds(t, width, stride=chunks), :] = jnp.where(
            lane < LANES - rest, parts[t], parts[t + 1]
        )

    unroll = 16

    @pl.loop(0, width // unroll)
    def _(group):
        for m in range(unroll):
            slot = group * unroll + m
            place = ids_ref[index * width + slot]
            rows[pl.ds(pl.multiple_of(place * chunks, chunks), chunks), :] = band[
                pl.ds(pl.multiple_of(slot * chunks, chunks), chunks), :
            ]


def whole_kernel(lags_ref, ids_ref, arrived_ref, weights_ref, out_ref, sources, band, rows):
    scatter_bands(lags_ref, ids_ref, arrived_ref, weights_ref, sources, band, rows)
    observers, out_len = out_ref.shape
    chunks = out_len // LANES

    @pl.when(pl.program_id(0) == pl.num_programs(0) - 1)
    def _():
        for t in range(chunks):
            out_ref[:, t * LANES : (t + 1) * LANES] = rows[pl.ds(t, observers, stride=chunks), :]


def banded_call(kernel, outs, arrived, kernel_weights, band_observers, band_lags):
    taps, terms, observers, faces = kernel_weights.shape
    bands, width = band_observers.shape
    steps = arrived.shape[-1]
    chunks = steps // 2 // LANES
    rank = len(arrived.shape)
    return pl.pallas_call(
        kernel,
        out_shape=outs,
        grid_spec=pltpu.PrefetchScalarGridSpec(
            num_scalar_prefetch=2,
            grid=(bands,),
            in_specs=[
                pl.BlockSpec(arrived.shape, lambda b, *_: (0,) * rank),
                pl.BlockSpec((taps, terms, width, faces), lambda b, *_: (0, 0, b, 0)),
            ],
            out_specs=jax.tree.map(
                lambda o: pl.BlockSpec(o.shape, lambda b, *_: (0,) * len(o.shape)), outs
            ),
            scratch_shapes=[
                pltpu.VMEM((taps * terms * faces, steps), jnp.bfloat16),
                pltpu.VMEM((width * chunks, LANES), jnp.float32),
                pltpu.VMEM((observers * chunks, LANES), jnp.float32),
            ],
        ),
        compiler_params=pltpu.CompilerParams(dimension_semantics=("arbitrary",)),
        name="bands",
    )(band_lags, band_observers.reshape(-1), arrived, kernel_weights)


def halve(total, axis, bit):
    size = lax.axis_size(axis)
    mine = (lax.axis_index(axis) >> bit) & 1
    if axis == "cfd":
        owners, rows, times = total.shape
        pairs = total.reshape(owners // 2, 2, rows, times)
        first, second = pairs[:, 0], pairs[:, 1]
    else:
        first, second = jnp.split(total, 2, axis=2)
    kept = jnp.where(mine == 1, second, first)
    sent = jnp.where(mine == 1, first, second).astype(jnp.bfloat16)
    partners = [(i, i ^ (1 << bit)) for i in range(size)]
    return kept + lax.ppermute(sent, axis, partners).astype(jnp.float32)


def exchange_sums(partial_value):
    owners = lax.axis_size("cfd")
    observers, times = partial_value.shape
    near = [("cfd", b) for b in range(owners.bit_length() - 1)]
    across = [("ac", b) for b in reversed(range(lax.axis_size("ac").bit_length() - 1))]
    orders = (near[:2] + across + near[2:], near[:1] + across + near[1:])
    total = halve(partial_value.reshape(owners, observers // owners, times), *near[0])
    streams = jnp.split(total, len(orders), axis=1)
    for step in range(1, len(near) + len(across)):
        streams = [halve(part, *order[step]) for part, order in zip(streams, orders)]
    return jnp.concatenate([part[0] for part in streams], axis=0)


def local(surface_raw, area_normals, kernel_weights, block_map, band_observers, band_lags):
    blocks = lax.axis_size("cfd")
    faces, steps = surface_raw.shape[1:]
    size = faces // blocks
    outgoing = prepare(surface_raw, area_normals, block_map[0, 0])
    arrived = lax.all_to_all(outgoing, "cfd", split_axis=0, concat_axis=0, tiled=True)
    arrived = arrived.reshape(blocks, 2, size, steps)
    if size % 8:
        arrived = arrived.transpose(1, 0, 2, 3).reshape(2 * faces, steps)
    partial_value = banded_call(
        whole_kernel,
        jax.ShapeDtypeStruct((kernel_weights.shape[2], steps // 2), jnp.float32),
        arrived,
        kernel_weights,
        band_observers,
        band_lags,
    )
    return exchange_sums(partial_value)


def solution(mesh):
    placed = (
        P(None, ("cfd", "ac"), None),
        P(None, ("cfd", "ac")),
        P(None, None, None, ("cfd", "ac")),
        P("ac", "cfd", None),
        P(),
        P(),
    )
    return jax.shard_map(
        local, mesh=mesh, in_specs=placed, out_specs=P("cfd", "ac"), check_vma=False
    )
```

```python
import functools

import jax
import jax.numpy as jnp
from jax import lax
from jax.experimental import pallas as pl
from jax.experimental.pallas import tpu as pltpu
from jax.sharding import PartitionSpec as P

LANES = 128


def prepare_kernel(src_ref, normals_ref, surface_ref, out_ref):
    along = surface_ref[2].astype(jnp.float32) * normals_ref[:, 0:1]
    along = along + surface_ref[3].astype(jnp.float32) * normals_ref[:, 1:2]
    along = along + surface_ref[4].astype(jnp.float32) * normals_ref[:, 2:3]
    thick = (surface_ref[1].astype(jnp.float32) * along).astype(jnp.bfloat16)
    both = jnp.concatenate([thick, surface_ref[0]], axis=0)
    rows = both.shape[0]
    column = lax.broadcasted_iota(jnp.int32, (rows, rows), 1)
    onehot = jnp.where(column == src_ref[...], 1.0, 0.0).astype(jnp.bfloat16)
    picked = jnp.dot(onehot, both, preferred_element_type=jnp.float32)
    out_ref[...] = picked.astype(jnp.bfloat16)


def prepare(surface_raw, area_normals, block_order):
    faces, steps = surface_raw.shape[1:]
    blocks = block_order.shape[0]
    size = faces // blocks
    src = (
        jnp.arange(2, dtype=jnp.int32)[None, :, None] * faces
        + block_order[:, None, None] * size
        + jnp.arange(size, dtype=jnp.int32)[None, None, :]
    ).reshape(2 * faces, 1)
    return pl.pallas_call(
        prepare_kernel,
        out_shape=jax.ShapeDtypeStruct((2 * faces, steps), jnp.bfloat16),
        name="prepare",
    )(src, area_normals.T.astype(jnp.float32), surface_raw)


def scatter_bands(lags_ref, ids_ref, arrived_ref, weights_ref, sources, band, rows):
    index = pl.program_id(0)
    taps, terms, width, faces = weights_ref.shape
    steps = sources.shape[1]
    out_len = steps // 2
    chunks = out_len // LANES

    @pl.when(index == 0)
    def _():
        series = arrived_ref[...].astype(jnp.float32)
        if len(arrived_ref.shape) == 4:
            thick = series[:, 0].reshape(faces, steps)
            pressure = series[:, 1].reshape(faces, steps)
        else:
            thick, pressure = series[:faces], series[faces:]
        step = lax.broadcasted_iota(jnp.int32, (faces, steps), 1)

        def rate(x):
            moved = jnp.where(step > 0, x - pltpu.roll(x, 1, 1), 0.0)
            return moved.astype(jnp.bfloat16).astype(jnp.float32)

        for c, x in enumerate((rate(thick), rate(pressure), pressure)):
            for k in range(taps):
                late = pltpu.roll(x, k, 1) if k else x
                sources[pl.ds((k * terms + c) * faces, faces), :] = late.astype(jnp.bfloat16)

    start = out_len - lags_ref[index]
    tile = jnp.minimum(start // LANES, steps // LANES - chunks - 1)
    rest = start - tile * LANES
    shift = lax.rem(LANES - rest, LANES)
    chosen = jnp.concatenate(
        [weights_ref[k, c] for k in range(taps) for c in range(terms)], axis=1
    )
    window = sources[:, pl.ds(pl.multiple_of(tile * LANES, LANES), out_len + LANES)]
    wide = jnp.dot(chosen, window, preferred_element_type=jnp.float32)
    lane = lax.broadcasted_iota(jnp.int32, (width, LANES), 1)
    parts = [
        pltpu.roll(wide[:, t * LANES : (t + 1) * LANES], shift, 1) for t in range(chunks + 1)
    ]
    for t in range(chunks):
        band[pl.ds(t, width, stride=chunks), :] = jnp.where(
            lane < LANES - rest, parts[t], parts[t + 1]
        )

    unroll = 32

    @pl.loop(0, width // unroll)
    def _(group):
        slots = [group * unroll + m for m in range(unroll)]
        places = [ids_ref[index * width + slot] for slot in slots]
        values = [
            band[pl.ds(pl.multiple_of(slot * chunks, chunks), chunks), :] for slot in slots
        ]
        for place, value in zip(places, values):
            rows[pl.ds(pl.multiple_of(place * chunks, chunks), chunks), :] = value


def whole_kernel(lags_ref, ids_ref, arrived_ref, weights_ref, out_ref, sources, band, rows):
    scatter_bands(lags_ref, ids_ref, arrived_ref, weights_ref, sources, band, rows)
    observers, out_len = out_ref.shape
    chunks = out_len // LANES

    @pl.when(pl.program_id(0) == pl.num_programs(0) - 1)
    def _():
        for t in range(chunks):
            out_ref[:, t * LANES : (t + 1) * LANES] = rows[pl.ds(t, observers, stride=chunks), :]


def banded_call(kernel, outs, arrived, kernel_weights, band_observers, band_lags):
    taps, terms, observers, faces = kernel_weights.shape
    bands, width = band_observers.shape
    steps = arrived.shape[-1]
    chunks = steps // 2 // LANES
    rank = len(arrived.shape)
    return pl.pallas_call(
        kernel,
        out_shape=outs,
        grid_spec=pltpu.PrefetchScalarGridSpec(
            num_scalar_prefetch=2,
            grid=(bands,),
            in_specs=[
                pl.BlockSpec(arrived.shape, lambda b, *_: (0,) * rank),
                pl.BlockSpec((taps, terms, width, faces), lambda b, *_: (0, 0, b, 0)),
            ],
            out_specs=jax.tree.map(
                lambda o: pl.BlockSpec(o.shape, lambda b, *_: (0,) * len(o.shape)), outs
            ),
            scratch_shapes=[
                pltpu.VMEM((taps * terms * faces, steps), jnp.bfloat16),
                pltpu.VMEM((width * chunks, LANES), jnp.float32),
                pltpu.VMEM((observers * chunks, LANES), jnp.float32),
            ],
        ),
        compiler_params=pltpu.CompilerParams(dimension_semantics=("arbitrary",)),
        name="bands",
    )(band_lags, band_observers.reshape(-1), arrived, kernel_weights)


def halve(total, axis, bit):
    size = lax.axis_size(axis)
    mine = (lax.axis_index(axis) >> bit) & 1
    if axis == "cfd":
        owners, rows, times = total.shape
        pairs = total.reshape(owners // 2, 2, rows, times)
        first, second = pairs[:, 0], pairs[:, 1]
    else:
        first, second = jnp.split(total, 2, axis=2)
    kept = jnp.where(mine == 1, second, first)
    sent = jnp.where(mine == 1, first, second).astype(jnp.bfloat16)
    partners = [(i, i ^ (1 << bit)) for i in range(size)]
    return kept + lax.ppermute(sent, axis, partners).astype(jnp.float32)


def exchange_sums(partial_value):
    owners = lax.axis_size("cfd")
    observers, times = partial_value.shape
    near = [("cfd", b) for b in range(owners.bit_length() - 1)]
    across = [("ac", b) for b in reversed(range(lax.axis_size("ac").bit_length() - 1))]
    orders = (near[:2] + across + near[2:], near[:1] + across + near[1:])
    total = halve(partial_value.reshape(owners, observers // owners, times), *near[0])
    streams = jnp.split(total, len(orders), axis=1)
    for step in range(1, len(near) + len(across)):
        streams = [halve(part, *order[step]) for part, order in zip(streams, orders)]
    return jnp.concatenate([part[0] for part in streams], axis=0)


def local(surface_raw, area_normals, kernel_weights, block_map, band_observers, band_lags):
    blocks = lax.axis_size("cfd")
    faces, steps = surface_raw.shape[1:]
    size = faces // blocks
    outgoing = prepare(surface_raw, area_normals, block_map[0, 0])
    arrived = lax.all_to_all(outgoing, "cfd", split_axis=0, concat_axis=0, tiled=True)
    arrived = arrived.reshape(blocks, 2, size, steps)
    if size % 8:
        arrived = arrived.transpose(1, 0, 2, 3).reshape(2 * faces, steps)
    partial_value = banded_call(
        whole_kernel,
        jax.ShapeDtypeStruct((kernel_weights.shape[2], steps // 2), jnp.float32),
        arrived,
        kernel_weights,
        band_observers,
        band_lags,
    )
    return exchange_sums(partial_value)


def solution(mesh):
    placed = (
        P(None, ("cfd", "ac"), None),
        P(None, ("cfd", "ac")),
        P(None, None, None, ("cfd", "ac")),
        P("ac", "cfd", None),
        P(),
        P(),
    )
    return jax.shard_map(
        local, mesh=mesh, in_specs=placed, out_specs=P("cfd", "ac"), check_vma=False
    )
```

```python
import functools

import jax
import jax.numpy as jnp
from jax import lax
from jax.experimental import pallas as pl
from jax.experimental.pallas import tpu as pltpu
from jax.sharding import PartitionSpec as P

LANES = 128


def prepare_kernel(src_ref, normals_ref, surface_ref, out_ref):
    along = surface_ref[2].astype(jnp.float32) * normals_ref[:, 0:1]
    along = along + surface_ref[3].astype(jnp.float32) * normals_ref[:, 1:2]
    along = along + surface_ref[4].astype(jnp.float32) * normals_ref[:, 2:3]
    thick = (surface_ref[1].astype(jnp.float32) * along).astype(jnp.bfloat16)
    both = jnp.concatenate([thick, surface_ref[0]], axis=0)
    rows = both.shape[0]
    column = lax.broadcasted_iota(jnp.int32, (rows, rows), 1)
    onehot = jnp.where(column == src_ref[...], 1.0, 0.0).astype(jnp.bfloat16)
    picked = jnp.dot(onehot, both, preferred_element_type=jnp.float32)
    out_ref[...] = picked.astype(jnp.bfloat16)


def prepare(surface_raw, area_normals, block_order):
    faces, steps = surface_raw.shape[1:]
    blocks = block_order.shape[0]
    size = faces // blocks
    src = (
        jnp.arange(2, dtype=jnp.int32)[None, :, None] * faces
        + block_order[:, None, None] * size
        + jnp.arange(size, dtype=jnp.int32)[None, None, :]
    ).reshape(2 * faces, 1)
    return pl.pallas_call(
        prepare_kernel,
        out_shape=jax.ShapeDtypeStruct((2 * faces, steps), jnp.bfloat16),
        name="prepare",
    )(src, area_normals.T.astype(jnp.float32), surface_raw)


def scatter_bands(lags_ref, ids_ref, arrived_ref, weights_ref, sources, band, rows):
    index = pl.program_id(0)
    taps, terms, width, faces = weights_ref.shape
    steps = sources.shape[1]
    out_len = steps // 2
    chunks = out_len // LANES

    @pl.when(index == 0)
    def _():
        series = arrived_ref[...].astype(jnp.float32)
        if len(arrived_ref.shape) == 4:
            thick = series[:, 0].reshape(faces, steps)
            pressure = series[:, 1].reshape(faces, steps)
        else:
            thick, pressure = series[:faces], series[faces:]
        step = lax.broadcasted_iota(jnp.int32, (faces, steps), 1)

        def rate(x):
            moved = jnp.where(step > 0, x - pltpu.roll(x, 1, 1), 0.0)
            return moved.astype(jnp.bfloat16).astype(jnp.float32)

        for c, x in enumerate((rate(thick), rate(pressure), pressure)):
            for k in range(taps):
                late = pltpu.roll(x, k, 1) if k else x
                sources[pl.ds((k * terms + c) * faces, faces), :] = late.astype(jnp.bfloat16)

    start = out_len - lags_ref[index]
    tile = jnp.minimum(start // LANES, steps // LANES - chunks - 1)
    rest = start - tile * LANES
    shift = lax.rem(LANES - rest, LANES)
    chosen = jnp.concatenate(
        [weights_ref[k, c] for k in range(taps) for c in range(terms)], axis=1
    )
    window = sources[:, pl.ds(pl.multiple_of(tile * LANES, LANES), out_len + LANES)]
    wide = jnp.dot(chosen, window, preferred_element_type=jnp.float32)
    lane = lax.broadcasted_iota(jnp.int32, (width, LANES), 1)
    parts = [
        pltpu.roll(wide[:, t * LANES : (t + 1) * LANES], shift, 1) for t in range(chunks + 1)
    ]
    for t in range(chunks):
        band[pl.ds(t, width, stride=chunks), :] = jnp.where(
            lane < LANES - rest, parts[t], parts[t + 1]
        )

    unroll = 32

    @pl.loop(0, width // unroll)
    def _(group):
        slots = [group * unroll + m for m in range(unroll)]
        places = [ids_ref[index * width + slot] for slot in slots]
        values = [
            band[pl.ds(pl.multiple_of(slot * chunks, chunks), chunks), :] for slot in slots
        ]
        for place, value in zip(places, values):
            rows[pl.ds(pl.multiple_of(place * chunks, chunks), chunks), :] = value


def halves_kernel(
    lags_ref, ids_ref, mine_ref, arrived_ref, weights_ref, kept_ref, sent_ref, sources, band, rows
):
    scatter_bands(lags_ref, ids_ref, arrived_ref, weights_ref, sources, band, rows)
    pairs, height, out_len = kept_ref.shape
    chunks = out_len // LANES
    mine = mine_ref[0]

    @pl.when(pl.program_id(0) == pl.num_programs(0) - 1)
    def _():
        for pair in range(pairs):
            for t in range(chunks):
                lanes = slice(t * LANES, (t + 1) * LANES)
                for out, owner in ((kept_ref, 2 * pair + mine), (sent_ref, 2 * pair + 1 - mine)):
                    first = pl.multiple_of(owner * (height * chunks), height * chunks)
                    part = rows[pl.ds(first + t, height, stride=chunks), :]
                    out[pair, :, lanes] = part.astype(out.dtype)


def banded_call(kernel, outs, arrived, kernel_weights, band_observers, band_lags, mine):
    taps, terms, observers, faces = kernel_weights.shape
    bands, width = band_observers.shape
    steps = arrived.shape[-1]
    chunks = steps // 2 // LANES
    rank = len(arrived.shape)
    return pl.pallas_call(
        kernel,
        out_shape=outs,
        grid_spec=pltpu.PrefetchScalarGridSpec(
            num_scalar_prefetch=3,
            grid=(bands,),
            in_specs=[
                pl.BlockSpec(arrived.shape, lambda b, *_: (0,) * rank),
                pl.BlockSpec((taps, terms, width, faces), lambda b, *_: (0, 0, b, 0)),
            ],
            out_specs=jax.tree.map(
                lambda o: pl.BlockSpec(o.shape, lambda b, *_: (0,) * len(o.shape)), outs
            ),
            scratch_shapes=[
                pltpu.VMEM((taps * terms * faces, steps), jnp.bfloat16),
                pltpu.VMEM((width * chunks, LANES), jnp.float32),
                pltpu.VMEM((observers * chunks, LANES), jnp.float32),
            ],
        ),
        compiler_params=pltpu.CompilerParams(dimension_semantics=("arbitrary",)),
        name="bands",
    )(band_lags, band_observers.reshape(-1), mine, arrived, kernel_weights)


def halve(total, axis, bit):
    size = lax.axis_size(axis)
    mine = (lax.axis_index(axis) >> bit) & 1
    if axis == "cfd":
        owners, rows, times = total.shape
        pairs = total.reshape(owners // 2, 2, rows, times)
        first, second = pairs[:, 0], pairs[:, 1]
    else:
        first, second = jnp.split(total, 2, axis=2)
    kept = jnp.where(mine == 1, second, first)
    sent = jnp.where(mine == 1, first, second).astype(jnp.bfloat16)
    partners = [(i, i ^ (1 << bit)) for i in range(size)]
    return kept + lax.ppermute(sent, axis, partners).astype(jnp.float32)


def exchange_sums(kept, sent):
    owners = lax.axis_size("cfd")
    near = [("cfd", b) for b in range(owners.bit_length() - 1)]
    across = [("ac", b) for b in reversed(range(lax.axis_size("ac").bit_length() - 1))]
    orders = (near[:2] + across + near[2:], near[:1] + across + near[1:])
    partners = [(i, i ^ 1) for i in range(owners)]
    total = kept + lax.ppermute(sent, "cfd", partners).astype(jnp.float32)
    streams = jnp.split(total, len(orders), axis=1)
    for step in range(1, len(near) + len(across)):
        streams = [halve(part, *order[step]) for part, order in zip(streams, orders)]
    return jnp.concatenate([part[0] for part in streams], axis=0)


def local(surface_raw, area_normals, kernel_weights, block_map, band_observers, band_lags):
    blocks = lax.axis_size("cfd")
    faces, steps = surface_raw.shape[1:]
    size = faces // blocks
    outgoing = prepare(surface_raw, area_normals, block_map[0, 0])
    arrived = lax.all_to_all(outgoing, "cfd", split_axis=0, concat_axis=0, tiled=True)
    arrived = arrived.reshape(blocks, 2, size, steps)
    if size % 8:
        arrived = arrived.transpose(1, 0, 2, 3).reshape(2 * faces, steps)
    shape = (blocks // 2, kernel_weights.shape[2] // blocks, steps // 2)
    kept, sent = banded_call(
        halves_kernel,
        [jax.ShapeDtypeStruct(shape, kind) for kind in (jnp.float32, jnp.bfloat16)],
        arrived,
        kernel_weights,
        band_observers,
        band_lags,
        (lax.axis_index("cfd") & 1).astype(jnp.int32).reshape(1),
    )
    return exchange_sums(kept, sent)


def solution(mesh):
    placed = (
        P(None, ("cfd", "ac"), None),
        P(None, ("cfd", "ac")),
        P(None, None, None, ("cfd", "ac")),
        P("ac", "cfd", None),
        P(),
        P(),
    )
    return jax.shard_map(
        local, mesh=mesh, in_specs=placed, out_specs=P("cfd", "ac"), check_vma=False
    )
```
